256 devices in a mesh: dp: 2 (over x_lo), space: 128 (over y, x_hi, z, core).
Axes of the slice: x: 4 (x_hi: 2, x_lo: 2; x = x_hi * 2 + x_lo), y: 4, z: 8, core: 2. Of those that a mesh axis runs over, the one named last changes fastest.
Arguments:
- activations: bfloat16 [4, 128, 64, 256], P('dp', 'space'), may hold values from -24 to 24
- out_grads: bfloat16 [4, 128, 64, 256], P('dp', 'space'), may hold values from -24 to 24
- old_input_factor: bfloat16 [2304, 2304], P(('dp', 'space')), may hold values from -3 to 3
- old_grad_factor: float32 [256, 256], P('space'), may hold values from -3 to 3
Outputs:
- input_factor: float32 [2304, 2304], P(('dp', 'space'))
- grad_factor: float32 [256, 256], P('space')
The draws below stay inside these ranges and needn't reach their ends.
All inputs are finite; a program needn't handle non-finite values.
Results may differ from the reference program's by a relative error of at most 0.00055.
Values may be sent and summed in bfloat16 or wider, within the bound.
No kernel may reach another device: no remote copies, remote signals or barrier semaphores. Data moves between devices by JAX's collectives and lax.ppermute only.
A program may use at most 128 MiB of HBM per device.

```python
import jax
import jax.numpy as jnp
from jax import lax

C = 256
KK = 2304
WIDTH = 64
BATCH = 4
HEIGHT = 128


def raised(entries, own_key, source, target, blocks, factor):
    def block_of(position):
        return (jnp.arange(entries.shape[position]) // (entries.shape[position] // blocks)).reshape((-1,) + (1,) * (entries.ndim - 1 - position))

    one_side = jax.random.permutation(own_key, blocks)[block_of(target)]
    far = (block_of(target) + blocks // 2) % blocks
    return jnp.where((block_of(source) == one_side) | (block_of(source) == far), factor * entries, entries)


def level_of(own_key, shape, split, low, high):
    def one(axis_at, blocks):
        heights = jax.random.uniform(jax.random.fold_in(jax.random.fold_in(own_key, 6), axis_at), (blocks,), jnp.float32, low / len(split), high / len(split))
        return jnp.repeat(jnp.exp(heights), shape[axis_at] // blocks).reshape((-1,) + (1,) * (len(shape) - axis_at - 1))

    gain = one(*split[0])
    for cut in split[1:]:
        gain = gain * one(*cut)
    return gain


def centred(stream_key, dims, spread, limit, shards=(), kind=jnp.bfloat16):
    array = spread * jax.random.normal(stream_key, dims, jnp.float32)
    if shards:
        array = array * level_of(stream_key, dims, shards, -0.22, 0.18)
    return jnp.clip(array, -limit, limit).astype(kind)


def noise_with(stream_key, dims, scale, limit, cuts, heavy, dtype=jnp.bfloat16):
    entries = scale * jax.random.normal(stream_key, dims, jnp.float32)
    if cuts:
        entries = entries * level_of(stream_key, dims, cuts, -0.22, 0.18)
    return jnp.clip(raised(entries, jax.random.fold_in(stream_key, 3), *heavy), -limit, limit).astype(dtype)


def setup_inputs(seed: int = 0) -> dict:
    arg_keys = jax.random.split(jax.random.key(seed), 5)
    return {
        "activations": noise_with(arg_keys[0], (BATCH, HEIGHT, WIDTH, C), 1.0, 24.0, ((0, 2), (1, 128)), (1, 3, 128, 5.5)),
        "out_grads": noise_with(arg_keys[1], (BATCH, HEIGHT, WIDTH, C), 1.0, 24.0, ((0, 2), (1, 128)), (1, 3, 128, 5.5)),
        "old_input_factor": centred(arg_keys[2], (KK, KK), 0.5, 3.0, ((0, 256),)),
        "old_grad_factor": centred(arg_keys[3], (C, C), 0.5, 3.0, ((0, 128),), jnp.float32),
    }


def patch_rows(image):
    height_now, width_now = image.shape[0], image.shape[1]
    padded = jnp.pad(image, ((1, 1), (1, 1), (0, 0)))
    pieces = [padded[ky:ky + height_now, kx:kx + width_now, :] for ky in range(3) for kx in range(3)]
    return jnp.concatenate(pieces, axis=2).reshape(height_now * width_now, -1)


def reference(activations, out_grads, old_input_factor, old_grad_factor):
    def step(carry, pair):
        image, grad_image = pair
        patches = patch_rows(image)
        flat = grad_image.reshape(-1, grad_image.shape[-1])
        input_part = lax.dot_general(patches, patches, (((0,), (0,)), ((), ())), preferred_element_type=jnp.float32)
        grad_part = lax.dot_general(flat, flat, (((0,), (0,)), ((), ())), preferred_element_type=jnp.float32)
        return (carry[0] + input_part, carry[1] + grad_part), None

    start = (jnp.zeros(old_input_factor.shape, jnp.float32), jnp.zeros(old_grad_factor.shape, jnp.float32))
    (input_sum, grad_sum), _ = lax.scan(step, start, (activations, out_grads))
    positions = activations.shape[0] * activations.shape[1] * activations.shape[2]
    input_factor = 0.5 * old_input_factor.astype(jnp.float32) + (0.5 / positions) * input_sum
    grad_factor = 0.5 * old_grad_factor + (0.5 / positions) * grad_sum
    return input_factor, grad_factor
```

```python
import jax
import jax.numpy as jnp
from jax import lax
from jax.experimental import pallas as pl
from jax.experimental.pallas import tpu as pltpu
from jax.sharding import Mesh
from jax.sharding import PartitionSpec as P

SPACE = ("y", "xh", "z", "c")
DP_SPACE = ("dp", "y", "xh", "z", "c")
Q = ("dp", "y", "xh")
ROW = 128
CH = 256
KK = 9 * CH
F32 = jnp.float32
BF16 = jnp.bfloat16
EXT = 512
WIDE = KK + EXT


def fan_kernel(a_ref, g_ref, out_ref, part):
    a = a_ref[...]
    g = g_ref[...]
    part[...] = lax.dot_general(g, g, (((0,), (0,)), ((), ())), preferred_element_type=F32)
    for z in range(8):
        out_ref[z, :ROW, :] = a
        rows = [part[32 * q + 4 * z : 32 * q + 4 * z + 4, :] for q in range(8)]
        out_ref[z, ROW:, :] = jnp.concatenate(rows, axis=0).astype(BF16)


def main_kernel(idx, got, oth, lo, hi, out, v, sel, lt, ext, gs):
    g = idx[0]
    c = idx[1]
    pos = lax.broadcasted_iota(jnp.int32, (ROW, CH), 0) % 64

    def put(x, row):
        at = pl.ds(pl.multiple_of(row * ROW, ROW), ROW)
        xf = x.astype(F32)
        v[1, at, :] = x
        v[0, at, :] = jnp.where(pos == 0, 0.0, pltpu.roll(xf, 1, 0)).astype(BF16)
        v[2, at, :] = jnp.where(pos == 63, 0.0, pltpu.roll(xf, ROW - 1, 0)).astype(BF16)

    put(lo[...], 0)
    put(hi[...], 17)

    def rows_of(z, carry):
        put(got[z, :ROW, :], 1 + 2 * z + c)
        put(oth[z, :ROW, :], 2 + 2 * z - c)
        return carry

    lax.fori_loop(0, 8, rows_of, 0)

    m = lax.broadcasted_iota(jnp.int32, (144, CH), 0)
    lane = lax.broadcasted_iota(jnp.int32, (144, CH), 1)
    owner = jnp.where(m < 128, m // 8, m - 128)
    within = jnp.where(m < 128, m % 8, 8)
    channel = owner * 144 + within + g * 9 - lane
    for t in range(9):
        sel[t] = jnp.where(channel == t * CH, 1.0, 0.0).astype(BF16)
    for n in range(8):
        acc = None
        for t in range(9):
            ky, kx = divmod(t, 3)
            part = lax.dot_general(
                sel[t],
                v[kx, ky * ROW + n * 256 : ky * ROW + n * 256 + 256, :],
                (((1,), (1,)), ((), ())),
                preferred_element_type=F32,
            )
            acc = part if acc is None else acc + part
        lt[:, n * 256 : n * 256 + 256] = acc.astype(BF16)

    ext[...] = jnp.zeros_like(ext)
    for t in range(9):
        ky, kx = divmod(t, 3)
        res = jnp.dot(lt[...], v[kx, ky * ROW : ky * ROW + 16 * ROW, :], preferred_element_type=F32)
        out[:, :, t * CH : t * CH + CH] = res[:128].reshape(16, 8, CH).astype(BF16)
        for q in range(16):
            ext[q, t // 2 : t // 2 + 1, (t % 2) * CH : (t % 2) * CH + CH] = res[128 + q : 129 + q]

    total = jnp.zeros((32, CH), F32)
    for z in range(8):
        total += got[z, ROW:, :].astype(F32) + oth[z, ROW:, :].astype(F32)
    gs[...] = total
    for q in range(16):
        for r in range(2):
            row = gs[pl.ds((q % 8) * 4 + r + 2 * c, 1), :]
            high = row.astype(BF16).astype(F32)
            ext[q, 5:6, r * CH : r * CH + CH] = high
            ext[q, 6:7, r * CH : r * CH + CH] = row - high
    out[:, :, KK:] = ext[...].astype(BF16)


def end_kernel(coef, got, old_in, old_g, out_in, out_g):
    total = got[0].astype(F32)
    for q in range(1, 16):
        total += got[q].astype(F32)
    out_in[0:8, :] = 0.5 * old_in[0:8, :].astype(F32) + coef * total[:, :KK]
    last = 0.5 * old_in[8:9, :].astype(F32)
    for i in range(9):
        at = KK + (i % 2) * CH
        out_in[8:9, i * CH : i * CH + CH] = (
            last[:, i * CH : i * CH + CH] + coef * total[i // 2 : i // 2 + 1, at : at + CH]
        )
    for r in range(2):
        at = KK + r * CH
        out_g[r : r + 1, :] = 0.5 * old_g[r : r + 1, :] + coef * (
            total[5:6, at : at + CH] + total[6:7, at : at + CH]
        )


def per_device(activations, out_grads, old_input_factor, old_grad_factor):
    images, rows_here, columns_here, channels = activations.shape
    positions = images * lax.axis_size("dp") * rows_here * lax.axis_size(SPACE) * columns_here
    a = activations.reshape(ROW, CH)
    g = out_grads.reshape(ROW, CH)
    c = lax.axis_index("c")
    index = jnp.stack([lax.axis_index("z") * 2 + c, c]).astype(jnp.int32)
    vmem = pl.BlockSpec(memory_space=pltpu.VMEM)
    smem = pl.BlockSpec(memory_space=pltpu.SMEM)
    sent = pl.pallas_call(
        fan_kernel,
        out_shape=jax.ShapeDtypeStruct((8, ROW + 32, CH), BF16),
        in_specs=[vmem, vmem],
        out_specs=vmem,
        scratch_shapes=[pltpu.VMEM((CH, CH), F32)],
    )(a, g)
    got = lax.all_to_all(sent, "z", 0, 0, tiled=True)
    oth = lax.ppermute(got, "c", [(0, 1), (1, 0)])
    first = jnp.where(c == 0, got[0, :ROW], oth[0, :ROW])
    last = jnp.where(c == 1, got[7, :ROW], oth[7, :ROW])
    lo = lax.ppermute(last, ("y", "xh"), [(i, i + 1) for i in range(7)])
    hi = lax.ppermute(first, ("y", "xh"), [(i + 1, i) for i in range(7)])
    parts = pl.pallas_call(
        main_kernel,
        out_shape=jax.ShapeDtypeStruct((16, 8, WIDE), BF16),
        in_specs=[smem, vmem, vmem, vmem, vmem],
        out_specs=vmem,
        scratch_shapes=[
            pltpu.VMEM((3, 18 * ROW, CH), BF16),
            pltpu.VMEM((9, 144, CH), BF16),
            pltpu.VMEM((144, 16 * ROW), BF16),
            pltpu.VMEM((16, 8, EXT), F32),
            pltpu.VMEM((32, CH), F32),
        ],
        cost_estimate=pl.CostEstimate(flops=3_000_000_000, bytes_accessed=3_000_000, transcendentals=0),
    )(index, got, oth, lo, hi)
    arrived = lax.all_to_all(parts, Q, 0, 0, tiled=True)
    return tuple(
        pl.pallas_call(
            lambda *refs: end_kernel(0.5 / positions, *refs),
            out_shape=(
                jax.ShapeDtypeStruct((9, KK), F32),
                jax.ShapeDtypeStruct((2, CH), F32),
            ),
            in_specs=[vmem, vmem, vmem],
            out_specs=(vmem, vmem),
        )(arrived, old_input_factor, old_grad_factor)
    )


def solution(mesh):
    finer = Mesh(
        mesh.devices.reshape(mesh.shape["dp"], 4, 2, 8, 2),
        ("dp", "y", "xh", "z", "c"),
    )
    return jax.shard_map(
        per_device,
        mesh=finer,
        in_specs=(
            P("dp", SPACE, None, None),
            P("dp", SPACE, None, None),
            P(DP_SPACE, None),
            P(SPACE, None),
        ),
        out_specs=(P(DP_SPACE, None), P(SPACE, None)),
        check_vma=False,
    )
```

```python
import jax
import jax.numpy as jnp
from jax import lax
from jax.experimental import pallas as pl
from jax.experimental.pallas import tpu as pltpu
from jax.sharding import Mesh
from jax.sharding import PartitionSpec as P


SPACE = ("y", "xh", "z", "c")
DP_SPACE = ("dp", "y", "xh", "z", "c")
Q = ("dp", "y", "xh")
ROW = 128
CH = 256
KK = 9 * CH
F32 = jnp.float32
BF16 = jnp.bfloat16
EXT = 512
WIDE = KK + EXT
M = 144

VMEM = pl.BlockSpec(memory_space=pltpu.VMEM)


def here():
    return lax.axis_index("z"), lax.axis_index("c")


def load_kernel(a, g, a_out, g_out, sems):
    copies = [pltpu.make_async_copy(x, y, sems.at[i]) for i, (x, y) in enumerate(((a, a_out), (g, g_out)))]
    for copy in copies:
        copy.start()
    for copy in copies:
        copy.wait()


def prep_kernel(a_own, a_oth, g_own, g_oth, out1, out2, mine, sums):
    z, c = here()
    a0 = a_own[...]
    a1 = a_oth[...]
    even = jnp.where(c == 0, a0, a1)
    odd = jnp.where(c == 0, a1, a0)
    g = jnp.concatenate([g_own[...], g_oth[...]], axis=0)
    i = lax.broadcasted_iota(jnp.int32, (CH, CH), 0)
    m = lax.broadcasted_iota(jnp.int32, (CH, CH), 1)
    source = 32 * ((m % 32) // 4) + 4 * (m // 32) + m % 4
    by_chip = jnp.where(i == source, 1.0, 0.0).astype(BF16)
    ordered = jnp.dot(g, by_chip, preferred_element_type=F32).astype(BF16)
    sums[...] = lax.dot_general(ordered, g, (((0,), (0,)), ((), ())), preferred_element_type=F32)

    def piece(chip):
        return sums[pl.ds(pl.multiple_of((chip % 8) * 32, 32), 32), :]

    step = 1 - 2 * c
    for d, out in ((1, out1), (2, out2)):
        out[:ROW, :] = even
        out[ROW : 2 * ROW, :] = odd
        out[2 * ROW : 2 * ROW + 32, :] = piece(z + 8 + d * step).astype(BF16)
        out[2 * ROW + 32 :, :] = piece(z + 8 + (d + 2) * step).astype(BF16)
    mine[...] = piece(z)


def shifts(x):
    pos = lax.broadcasted_iota(jnp.int32, (ROW, CH), 0) % 64
    xf = x.astype(F32)
    return (
        jnp.where(pos == 0, 0.0, pltpu.roll(xf, 1, 0)).astype(BF16),
        x,
        jnp.where(pos == 63, 0.0, pltpu.roll(xf, ROW - 1, 0)).astype(BF16),
    )


def selection(t):
    z, c = here()
    m = lax.broadcasted_iota(jnp.int32, (M, CH), 0)
    lane = lax.broadcasted_iota(jnp.int32, (M, CH), 1)
    owner = jnp.where(m < 128, m // 8, m - 128)
    within = jnp.where(m < 128, m % 8, 8)
    channel = owner * M + within + (z * 2 + c) * 9 - lane
    return jnp.where(channel == t * CH, 1.0, 0.0).astype(BF16)


def nt(a, b):
    return lax.dot_general(a, b, (((1,), (1,)), ((), ())), preferred_element_type=F32)


def main_kernel(a_own, a_oth, r1, s1, r2, s2, r3, s3, r4, s4, mine, out, v, sel, lt, ext, gs):
    z, c = here()
    chip = (lax.axis_index("y") * 2 + lax.axis_index("xh")) * 8 + z
    step = 1 - 2 * c

    def put(x, row):
        at = pl.ds(pl.multiple_of(row * ROW, ROW), ROW)
        for kx, moved in enumerate(shifts(x)):
            v[kx, at, :] = moved

    put(a_own[...], 8 + c)
    put(a_oth[...], 9 - c)
    for d, r, s in ((1, r1, s1), (2, r2, s2), (3, r3, s3), (4, r4, s4)):
        for half in range(2):
            put(r[half * ROW : half * ROW + ROW, :], 8 - 2 * d * step + half)
            put(s[half * ROW : half * ROW + ROW, :], 8 + 2 * d * step + half)
    for t in range(9):
        sel[t] = selection(t)
    top = (7 - 2 * chip + 128) % 128
    bottom = (6 - 2 * chip + 128) % 128
    lane = lax.broadcasted_iota(jnp.int32, (M, 256), 1)
    for n in range(8):
        sums = []
        for ky in range(3):
            acc = None
            for kx in range(3):
                part = nt(sel[3 * ky + kx], v[kx, ky * ROW + n * 256 : ky * ROW + n * 256 + 256, :])
                acc = part if acc is None else acc + part
            sums.append(acc)
        row = 2 * n + lane // ROW
        at_top = row == top
        at_bottom = row == bottom
        left = jnp.where(at_top, 0.0, sums[0]) + sums[1] + jnp.where(at_bottom, 0.0, sums[2])
        lanes = slice(n * 256, n * 256 + 256)
        lt[0, :, lanes] = jnp.where(at_top, 0.0, left).astype(BF16)
        lt[1, :, lanes] = left.astype(BF16)
        lt[2, :, lanes] = jnp.where(at_bottom, 0.0, left).astype(BF16)
    ext[...] = jnp.zeros_like(ext)
    for t in range(9):
        ky, kx = divmod(t, 3)
        res = jnp.dot(lt[ky], v[kx, ky * ROW : ky * ROW + 16 * ROW, :], preferred_element_type=F32)
        out[:, :, t * CH : t * CH + CH] = res[:128].reshape(16, 8, CH).astype(BF16)
        for q in range(16):
            ext[q, t // 2 : t // 2 + 1, (t % 2) * CH : (t % 2) * CH + CH] = res[128 + q : 129 + q]
    near = slice(2 * ROW, 2 * ROW + 32)
    far = slice(2 * ROW + 32, 2 * ROW + 64)
    total = mine[...]
    for ref, rows in ((r1, near), (s1, near), (r2, near), (s2, near), (r3, far), (s3, far)):
        total += ref[rows, :].astype(F32)
    gs[...] = total + jnp.where(c == 0, r4[far, :].astype(F32), s4[far, :].astype(F32))
    for q in range(8):
        for r in range(2):
            row = gs[pl.ds(q * 4 + r + 2 * c, 1), :]
            high = row.astype(BF16).astype(F32)
            for group in (0, 8):
                ext[group + q, 5:6, r * CH : r * CH + CH] = high
                ext[group + q, 6:7, r * CH : r * CH + CH] = row - high
    out[:, :, KK:] = ext[...].astype(BF16)


def end_kernel(coef, got, old_in, old_g, out_in, out_g):
    total = got[0].astype(F32)
    for q in range(1, 16):
        total += got[q].astype(F32)
    out_in[0:8, :] = 0.5 * old_in[0:8, :].astype(F32) + coef * total[:, :KK]
    last = 0.5 * old_in[8:9, :].astype(F32)
    for i in range(9):
        at = KK + (i % 2) * CH
        out_in[8:9, i * CH : i * CH + CH] = (
            last[:, i * CH : i * CH + CH] + coef * total[i // 2 : i // 2 + 1, at : at + CH]
        )
    for r in range(2):
        at = KK + r * CH
        out_g[r : r + 1, :] = 0.5 * old_g[r : r + 1, :] + coef * (
            total[5:6, at : at + CH] + total[6:7, at : at + CH]
        )


def call(kernel, shapes, args, scratch=(), flops=0, mib=8):
    return pl.pallas_call(
        kernel,
        out_shape=[jax.ShapeDtypeStruct(s, d) for s, d in shapes],
        in_specs=[VMEM] * len(args),
        out_specs=[VMEM] * len(shapes),
        scratch_shapes=[pltpu.VMEM(s, d) for s, d in scratch],
        cost_estimate=pl.CostEstimate(flops=flops, bytes_accessed=flops // 1000, transcendentals=0),
        compiler_params=pltpu.CompilerParams(vmem_limit_bytes=mib * 2**20),
    )(*args)


def swap(x):
    return lax.ppermute(x, "c", [(0, 1), (1, 0)])


def along(x, d):
    pairs = []
    for chip in range(64):
        pairs.append((2 * chip, 2 * ((chip + d) % 64)))
        pairs.append((2 * chip + 1, 2 * ((chip - d) % 64) + 1))
    return lax.ppermute(x, SPACE, pairs)


def per_device(activations, out_grads, old_input_factor, old_grad_factor):
    images, rows_here, columns_here, _ = activations.shape
    positions = images * lax.axis_size("dp") * rows_here * lax.axis_size(SPACE) * columns_here
    a = activations.reshape(ROW, CH)
    g = out_grads.reshape(ROW, CH)
    a_oth = swap(a)
    g_oth = swap(g)
    a_own, g_own = pl.pallas_call(
        load_kernel,
        out_shape=[jax.ShapeDtypeStruct((ROW, CH), BF16)] * 2,
        in_specs=[pl.BlockSpec(memory_space=pltpu.HBM)] * 2,
        out_specs=[VMEM] * 2,
        scratch_shapes=[pltpu.SemaphoreType.DMA((2,))],
        compiler_params=pltpu.CompilerParams(vmem_limit_bytes=2**20),
        name="load",
    )(a, g)
    sent1, sent2, mine = call(
        prep_kernel,
        [((320, CH), BF16)] * 2 + [((32, CH), F32)],
        (a_own, a_oth, g_own, g_oth),
        scratch=[((CH, CH), F32)],
        flops=1_000_000_000,
    )
    r1 = along(sent1, 1)
    r2 = along(sent2, 2)
    r3 = along(r1, 2)
    r4 = along(r2, 2)
    moved = []
    for r in (r1, r2, r3, r4):
        moved += [r, swap(r)]
    (parts,) = call(
        main_kernel,
        [((16, 8, WIDE), BF16)],
        (a_own, a_oth, *moved, mine),
        scratch=[
            ((3, 18 * ROW, CH), BF16),
            ((9, M, CH), BF16),
            ((3, M, 16 * ROW), BF16),
            ((16, 8, EXT), F32),
            ((32, CH), F32),
        ],
        flops=4_000_000_000,
        mib=24,
    )
    arrived = lax.all_to_all(parts, Q, 0, 0, tiled=True)
    return tuple(
        call(
            lambda *refs: end_kernel(0.5 / positions, *refs),
            [((9, KK), F32), ((2, CH), F32)],
            (arrived, old_input_factor, old_grad_factor),
        )
    )


def solution(mesh):
    finer = Mesh(
        mesh.devices.reshape(mesh.shape["dp"], 4, 2, 8, 2),
        ("dp", "y", "xh", "z", "c"),
    )

    return jax.shard_map(
        per_device,
        mesh=finer,
        in_specs=(
            P("dp", SPACE, None, None),
            P("dp", SPACE, None, None),
            P(DP_SPACE, None),
            P(SPACE, None),
        ),
        out_specs=(P(DP_SPACE, None), P(SPACE, None)),
        check_vma=False,
    )
```

```python
import jax
import jax.numpy as jnp
from jax import lax
from jax.experimental import pallas as pl
from jax.experimental.pallas import tpu as pltpu
from jax.sharding import Mesh
from jax.sharding import PartitionSpec as P


SPACE = ("y", "xh", "z", "c")
DP_SPACE = ("dp", "y", "xh", "z", "c")
Q = ("dp", "y", "xh")
ROW = 128
CH = 256
KK = 9 * CH
F32 = jnp.float32
BF16 = jnp.bfloat16
EXT = 512
WIDE = KK + EXT
M = 144

VMEM = pl.BlockSpec(memory_space=pltpu.VMEM)


def here():
    return lax.axis_index("z"), lax.axis_index("c")


def prep_kernel(own, a_oth, g_oth, out1, out2, out3, pair, mine, sums):
    z, c = here()
    a0 = own[:ROW, :]
    a1 = a_oth[...]
    even = jnp.where(c == 0, a0, a1)
    odd = jnp.where(c == 0, a1, a0)
    g = jnp.concatenate([own[ROW:, :], g_oth[...]], axis=0)
    i = lax.broadcasted_iota(jnp.int32, (CH, CH), 0)
    m = lax.broadcasted_iota(jnp.int32, (CH, CH), 1)
    source = 32 * ((m % 32) // 4) + 4 * (m // 32) + m % 4
    by_chip = jnp.where(i == source, 1.0, 0.0).astype(BF16)
    ordered = jnp.dot(g, by_chip, preferred_element_type=F32).astype(BF16)
    sums[...] = lax.dot_general(ordered, g, (((0,), (0,)), ((), ())), preferred_element_type=F32)

    def piece(chip):
        return sums[pl.ds(pl.multiple_of((chip % 8) * 32, 32), 32), :]

    step = 1 - 2 * c
    for d, out in ((1, out1), (2, out2), (3, out3)):
        out[:ROW, :] = even
        out[ROW : 2 * ROW, :] = odd
        out[2 * ROW : 2 * ROW + 32, :] = piece(z + 8 + d * step).astype(BF16)
    out2[2 * ROW + 32 :, :] = piece(z + 8 + 4 * step).astype(BF16)
    pair[:ROW, :] = even
    pair[ROW:, :] = odd
    mine[...] = piece(z)


def shifts(x):
    pos = lax.broadcasted_iota(jnp.int32, (ROW, CH), 0) % 64
    xf = x.astype(F32)
    return (
        jnp.where(pos == 0, 0.0, pltpu.roll(xf, 1, 0)).astype(BF16),
        x,
        jnp.where(pos == 63, 0.0, pltpu.roll(xf, ROW - 1, 0)).astype(BF16),
    )


def selection(t):
    z, c = here()
    m = lax.broadcasted_iota(jnp.int32, (2 * M, CH), 0)
    lane = lax.broadcasted_iota(jnp.int32, (2 * M, CH), 1)
    core = jnp.where(m < M, c, 1 - c)
    m = jnp.where(m < M, m, m - M)
    owner = jnp.where(m < 128, m // 8, m - 128)
    within = jnp.where(m < 128, m % 8, 8)
    channel = owner * M + within + (z * 2 + core) * 9 - lane
    return jnp.where(channel == t * CH, 1.0, 0.0).astype(BF16)


def nt(a, b):
    return lax.dot_general(a, b, (((1,), (1,)), ((), ())), preferred_element_type=F32)


def fill(pairs, v):
    c = lax.axis_index("c")
    for i, pair in enumerate(pairs):
        at = jnp.where(c == 0, len(pairs) - 1 - i, i)
        for half in range(2):
            where = pl.ds(pl.multiple_of((2 * at + half) * ROW, ROW), ROW)
            for kx, moved in enumerate(shifts(pair[half * ROW : half * ROW + ROW, :])):
                v[kx, where, :] = moved


def left_side(near, pairs, v, sel, lt):
    z, c = here()
    chip = (lax.axis_index("y") * 2 + lax.axis_index("xh")) * 8 + z
    patches = 2 * pairs - 2
    start = 2 * chip + 1 + jnp.where(c == 0, -2 * (near + pairs - 1), 2 * near)
    top = (256 - start) % 128
    bottom = (255 - start) % 128
    lane = lax.broadcasted_iota(jnp.int32, (2 * M, 256), 1)
    for n in range(patches // 2):
        sums = []
        for ky in range(3):
            acc = None
            for kx in range(3):
                part = nt(sel[3 * ky + kx], v[kx, ky * ROW + n * 256 : ky * ROW + n * 256 + 256, :])
                acc = part if acc is None else acc + part
            sums.append(acc)
        row = 2 * n + lane // ROW
        at_top = row == top
        at_bottom = row == bottom
        left = jnp.where(at_top, 0.0, sums[0]) + sums[1] + jnp.where(at_bottom, 0.0, sums[2])
        lanes = slice(n * 256, n * 256 + 256)
        lt[0, :, lanes] = jnp.where(at_top, 0.0, left).astype(BF16)
        lt[1, :, lanes] = left.astype(BF16)
        lt[2, :, lanes] = jnp.where(at_bottom, 0.0, left).astype(BF16)


def product(t, patches, v, lt):
    ky, kx = divmod(t, 3)
    return jnp.dot(lt[ky], v[kx, ky * ROW : (ky + patches) * ROW, :], preferred_element_type=F32)


def near_kernel(pair, r1, r2, acc, sel, v, lt):
    fill((pair, r1, r2), v)
    for t in range(9):
        sel[t] = selection(t)
    left_side(0, 3, v, sel, lt)
    for t in range(9):
        acc[:, t * CH : t * CH + CH] = product(t, 4, v, lt)


def middle_kernel(r2, r3, sel, old, acc, v, lt):
    fill((r2, r3), v)
    left_side(2, 2, v, sel, lt)
    for t in range(9):
        lanes = slice(t * CH, t * CH + CH)
        acc[:, lanes] = old[:, lanes] + product(t, 2, v, lt)


def far_kernel(r1, r2, r3, r4, mine, sel, old, keep, give, v, lt, ext, gs):
    c = lax.axis_index("c")
    fill((r3, r4), v)
    left_side(3, 2, v, sel, lt)
    ext[...] = jnp.zeros_like(ext)
    for t in range(9):
        lanes = slice(t * CH, t * CH + CH)
        res = old[:, lanes] + product(t, 2, v, lt)
        keep[:, :, lanes] = res[:128].reshape(16, 8, CH)
        give[:, :, lanes] = res[M : M + 128].reshape(16, 8, CH).astype(BF16)
        lanes = slice((t % 2) * CH, (t % 2) * CH + CH)
        for side in range(2):
            for q in range(16):
                at = side * M + 128 + q
                ext[side, q, t // 2 : t // 2 + 1, lanes] = res[at : at + 1]
    total = jnp.where(c == 0, mine[...], 0.0)
    for ref in (r1, r2, r3):
        total += ref[2 * ROW : 2 * ROW + 32, :].astype(F32)
    gs[...] = total + jnp.where(c == 0, r4[2 * ROW + 32 :, :].astype(F32), 0.0)
    for side in range(2):
        core = c if side == 0 else 1 - c
        for q in range(8):
            for r in range(2):
                row = gs[pl.ds(q * 4 + r + 2 * core, 1), :]
                high = row.astype(BF16).astype(F32)
                for group in (0, 8):
                    ext[side, group + q, 5:6, r * CH : r * CH + CH] = high
                    ext[side, group + q, 6:7, r * CH : r * CH + CH] = row - high
    keep[:, :, KK:] = ext[0]
    give[:, :, KK:] = ext[1].astype(BF16)


def join_kernel(keep, got, out):
    for q in range(16):
        total = keep[q] + got[q].astype(F32)
        out[q, :, :] = total.astype(BF16)
        grad = total[5:6, KK:] + total[6:7, KK:]
        high = grad.astype(BF16).astype(F32)
        row = lax.broadcasted_iota(jnp.int32, (8, EXT), 0)
        tail = jnp.where(row == 5, high, jnp.where(row == 6, grad - high, total[:, KK:]))
        out[q, :, KK:] = tail.astype(BF16)


def end_kernel(coef, got, old_in, old_g, out_in, out_g):
    total = got[0].astype(F32)
    for q in range(1, 16):
        total += got[q].astype(F32)
    out_in[0:8, :] = 0.5 * old_in[0:8, :].astype(F32) + coef * total[:, :KK]
    last = 0.5 * old_in[8:9, :].astype(F32)
    for i in range(9):
        at = KK + (i % 2) * CH
        out_in[8:9, i * CH : i * CH + CH] = (
            last[:, i * CH : i * CH + CH] + coef * total[i // 2 : i // 2 + 1, at : at + CH]
        )
    for r in range(2):
        at = KK + r * CH
        out_g[r : r + 1, :] = 0.5 * old_g[r : r + 1, :] + coef * (
            total[5:6, at : at + CH] + total[6:7, at : at + CH]
        )


def call(kernel, shapes, args, scratch=(), flops=0, mib=8):
    return pl.pallas_call(
        kernel,
        out_shape=[jax.ShapeDtypeStruct(s, d) for s, d in shapes],
        in_specs=[VMEM] * len(args),
        out_specs=[VMEM] * len(shapes),
        scratch_shapes=[pltpu.VMEM(s, d) for s, d in scratch],
        cost_estimate=pl.CostEstimate(flops=flops, bytes_accessed=flops // 1000, transcendentals=0),
        compiler_params=pltpu.CompilerParams(vmem_limit_bytes=mib * 2**20),
    )(*args)


def swap(x):
    return lax.ppermute(x, "c", [(0, 1), (1, 0)])


def along(x, d):
    pairs = []
    for chip in range(64):
        pairs.append((2 * chip, 2 * ((chip + d) % 64)))
        pairs.append((2 * chip + 1, 2 * ((chip - d) % 64) + 1))
    return lax.ppermute(x, SPACE, pairs)


def per_device(activations, out_grads, old_input_factor, old_grad_factor):
    images, rows_here, columns_here, _ = activations.shape
    positions = images * lax.axis_size("dp") * rows_here * lax.axis_size(SPACE) * columns_here
    a = activations.reshape(ROW, CH)
    g = out_grads.reshape(ROW, CH)
    a_oth = swap(a)
    g_oth = swap(g)
    own = jnp.concatenate([a, g], axis=0)
    *sent, pair, mine = call(
        prep_kernel,
        [((rows, CH), BF16) for rows in (288, 320, 288, 2 * ROW)] + [((32, CH), F32)],
        (own, a_oth, g_oth),
        scratch=[((CH, CH), F32)],
        flops=1_000_000_000,
    )
    moved = [along(x, d) for d, x in enumerate(sent, 1)]
    moved.append(along(moved[1], 2))
    r1, r2, r3, r4 = moved
    acc, sel = call(
        near_kernel,
        [((2 * M, KK), F32), ((9, 2 * M, CH), BF16)],
        (pair, r1, r2),
        scratch=[((3, 6 * ROW, CH), BF16), ((3, 2 * M, 4 * ROW), BF16)],
        flops=2_000_000_000,
        mib=16,
    )
    (acc,) = call(
        middle_kernel,
        [((2 * M, KK), F32)],
        (r2, r3, sel, acc),
        scratch=[((3, 4 * ROW, CH), BF16), ((3, 2 * M, 2 * ROW), BF16)],
        flops=1_000_000_000,
        mib=16,
    )
    keep, give = call(
        far_kernel,
        [((16, 8, WIDE), F32), ((16, 8, WIDE), BF16)],
        (r1, r2, r3, r4, mine, sel, acc),
        scratch=[
            ((3, 4 * ROW, CH), BF16),
            ((3, 2 * M, 2 * ROW), BF16),
            ((2, 16, 8, EXT), F32),
            ((32, CH), F32),
        ],
        flops=1_000_000_000,
        mib=18,
    )
    got = swap(give)
    (parts,) = call(join_kernel, [((16, 8, WIDE), BF16)], (keep, got))
    arrived = lax.all_to_all(parts, Q, 0, 0, tiled=True)
    return tuple(
        call(
            lambda *refs: end_kernel(0.5 / positions, *refs),
            [((9, KK), F32), ((2, CH), F32)],
            (arrived, old_input_factor, old_grad_factor),
        )
    )


def solution(mesh):
    finer = Mesh(
        mesh.devices.reshape(mesh.shape["dp"], 4, 2, 8, 2),
        ("dp", "y", "xh", "z", "c"),
    )

    return jax.shard_map(
        per_device,
        mesh=finer,
        in_specs=(
            P("dp", SPACE, None, None),
            P("dp", SPACE, None, None),
            P(DP_SPACE, None),
            P(SPACE, None),
        ),
        out_specs=(P(DP_SPACE, None), P(SPACE, None)),
        check_vma=False,
    )
```

```python
import jax
import jax.numpy as jnp
from jax import lax
from jax.experimental import pallas as pl
from jax.experimental.pallas import tpu as pltpu
from jax.sharding import Mesh
from jax.sharding import PartitionSpec as P


SPACE = ("y", "xh", "z", "c")
DP_SPACE = ("dp", "y", "xh", "z", "c")
Q = ("dp", "y", "xh")
ROW = 128
CH = 256
KK = 9 * CH
F32 = jnp.float32
BF16 = jnp.bfloat16
EXT = 512
WIDE = KK + EXT
M = 144

VMEM = pl.BlockSpec(memory_space=pltpu.VMEM)


def here():
    return lax.axis_index("z"), lax.axis_index("c")


def prep_kernel(own, a_oth, g_oth, out1, out2, out3, pair, mine, sums):
    z, c = here()
    a0 = own[:ROW, :]
    a1 = a_oth[...]
    even = jnp.where(c == 0, a0, a1)
    odd = jnp.where(c == 0, a1, a0)
    g = jnp.concatenate([own[ROW:, :], g_oth[...]], axis=0)
    i = lax.broadcasted_iota(jnp.int32, (CH, CH), 0)
    m = lax.broadcasted_iota(jnp.int32, (CH, CH), 1)
    source = 32 * ((m % 32) // 4) + 4 * (m // 32) + m % 4
    by_chip = jnp.where(i == source, 1.0, 0.0).astype(BF16)
    ordered = jnp.dot(g, by_chip, preferred_element_type=F32).astype(BF16)
    sums[...] = lax.dot_general(ordered, g, (((0,), (0,)), ((), ())), preferred_element_type=F32)

    def piece(chip):
        return sums[pl.ds(pl.multiple_of((chip % 8) * 32, 32), 32), :]

    step = 1 - 2 * c
    for d, out in ((1, out1), (2, out2), (3, out3)):
        out[:ROW, :] = even
        out[ROW : 2 * ROW, :] = odd
        out[2 * ROW : 2 * ROW + 32, :] = piece(z + 8 + d * step).astype(BF16)
    out2[2 * ROW + 32 :, :] = piece(z + 8 + 4 * step).astype(BF16)
    pair[:ROW, :] = even
    pair[ROW:, :] = odd
    mine[...] = piece(z)


def shifts(x):
    pos = lax.broadcasted_iota(jnp.int32, (ROW, CH), 0) % 64
    xf = x.astype(F32)
    return (
        jnp.where(pos == 0, 0.0, pltpu.roll(xf, 1, 0)).astype(BF16),
        x,
        jnp.where(pos == 63, 0.0, pltpu.roll(xf, ROW - 1, 0)).astype(BF16),
    )


def selection(t):
    z, c = here()
    m = lax.broadcasted_iota(jnp.int32, (2 * M, CH), 0)
    lane = lax.broadcasted_iota(jnp.int32, (2 * M, CH), 1)
    core = jnp.where(m < M, c, 1 - c)
    m = jnp.where(m < M, m, m - M)
    owner = jnp.where(m < 128, m // 8, m - 128)
    within = jnp.where(m < 128, m % 8, 8)
    channel = owner * M + within + (z * 2 + core) * 9 - lane
    return jnp.where(channel == t * CH, 1.0, 0.0).astype(BF16)


def nt(a, b):
    return lax.dot_general(a, b, (((1,), (1,)), ((), ())), preferred_element_type=F32)


def fill(pairs, v):
    c = lax.axis_index("c")
    for i, pair in enumerate(pairs):
        at = jnp.where(c == 0, len(pairs) - 1 - i, i)
        for half in range(2):
            where = pl.ds(pl.multiple_of((2 * at + half) * ROW, ROW), ROW)
            for kx, moved in enumerate(shifts(pair[half * ROW : half * ROW + ROW, :])):
                v[kx, where, :] = moved


def left_side(near, pairs, v, sel, lt, first=0, count=2 * M):
    z, c = here()
    chip = (lax.axis_index("y") * 2 + lax.axis_index("xh")) * 8 + z
    patches = 2 * pairs - 2
    start = 2 * chip + 1 + jnp.where(c == 0, -2 * (near + pairs - 1), 2 * near)
    top = (256 - start) % 128
    bottom = (255 - start) % 128
    lane = lax.broadcasted_iota(jnp.int32, (count, 256), 1)
    for n in range(patches // 2):
        sums = []
        for ky in range(3):
            acc = None
            for kx in range(3):
                part = nt(
                    sel[3 * ky + kx, first : first + count, :],
                    v[kx, ky * ROW + n * 256 : ky * ROW + n * 256 + 256, :],
                )
                acc = part if acc is None else acc + part
            sums.append(acc)
        row = 2 * n + lane // ROW
        at_top = row == top
        at_bottom = row == bottom
        left = jnp.where(at_top, 0.0, sums[0]) + sums[1] + jnp.where(at_bottom, 0.0, sums[2])
        lanes = slice(n * 256, n * 256 + 256)
        lt[0, :, lanes] = jnp.where(at_top, 0.0, left).astype(BF16)
        lt[1, :, lanes] = left.astype(BF16)
        lt[2, :, lanes] = jnp.where(at_bottom, 0.0, left).astype(BF16)


def product(t, patches, v, lt):
    ky, kx = divmod(t, 3)
    return jnp.dot(lt[ky], v[kx, ky * ROW : (ky + patches) * ROW, :], preferred_element_type=F32)


def near_kernel(pair, r1, r2, acc, sel, v, lt):
    fill((pair, r1, r2), v)
    for t in range(9):
        sel[t] = selection(t)
    left_side(0, 3, v, sel, lt)
    for t in range(9):
        acc[:, t * CH : t * CH + CH] = product(t, 4, v, lt)


def middle_kernel(r2, r3, sel, old, acc, v, lt):
    fill((r2, r3), v)
    left_side(2, 2, v, sel, lt)
    for t in range(9):
        lanes = slice(t * CH, t * CH + CH)
        acc[:, lanes] = old[:, lanes] + product(t, 2, v, lt)


def far_give_kernel(r1, r2, r3, r4, mine, sel, old, give, v, gs, lt, ext):
    c = lax.axis_index("c")
    fill((r3, r4), v)
    left_side(3, 2, v, sel, lt, M, M)
    total = jnp.where(c == 0, mine[...], 0.0)
    for ref in (r1, r2, r3):
        total += ref[2 * ROW : 2 * ROW + 32, :].astype(F32)
    gs[...] = total + jnp.where(c == 0, r4[2 * ROW + 32 :, :].astype(F32), 0.0)
    finish(1 - c, M, old, v, lt, gs, give, ext)


def far_keep_kernel(sel, old, v, gs, keep, lt, ext):
    left_side(3, 2, v, sel, lt, 0, M)
    finish(lax.axis_index("c"), 0, old, v, lt, gs, keep, ext)


def finish(core, first, old, v, lt, gs, out, ext):
    ext[...] = jnp.zeros_like(ext)
    for t in range(9):
        lanes = slice(t * CH, t * CH + CH)
        res = old[first : first + M, lanes] + product(t, 2, v, lt)
        out[:, :, lanes] = res[:128].reshape(16, 8, CH).astype(out.dtype)
        lanes = slice((t % 2) * CH, (t % 2) * CH + CH)
        for q in range(16):
            ext[q, t // 2 : t // 2 + 1, lanes] = res[128 + q : 129 + q]
    for q in range(8):
        for r in range(2):
            row = gs[pl.ds(q * 4 + r + 2 * core, 1), :]
            high = row.astype(BF16).astype(F32)
            for group in (0, 8):
                ext[group + q, 5:6, r * CH : r * CH + CH] = high
                ext[group + q, 6:7, r * CH : r * CH + CH] = row - high
    out[:, :, KK:] = ext[...].astype(out.dtype)


def join_kernel(keep, got, out):
    for q in range(16):
        total = keep[q] + got[q].astype(F32)
        out[q, :, :] = total.astype(BF16)
        grad = total[5:6, KK:] + total[6:7, KK:]
        high = grad.astype(BF16).astype(F32)
        row = lax.broadcasted_iota(jnp.int32, (8, EXT), 0)
        tail = jnp.where(row == 5, high, jnp.where(row == 6, grad - high, total[:, KK:]))
        out[q, :, KK:] = tail.astype(BF16)


def end_kernel(coef, got, old_in, old_g, out_in, out_g):
    total = got[0].astype(F32)
    for q in range(1, 16):
        total += got[q].astype(F32)
    out_in[0:8, :] = 0.5 * old_in[0:8, :].astype(F32) + coef * total[:, :KK]
    last = 0.5 * old_in[8:9, :].astype(F32)
    for i in range(9):
        at = KK + (i % 2) * CH
        out_in[8:9, i * CH : i * CH + CH] = (
            last[:, i * CH : i * CH + CH] + coef * total[i // 2 : i // 2 + 1, at : at + CH]
        )
    for r in range(2):
        at = KK + r * CH
        out_g[r : r + 1, :] = 0.5 * old_g[r : r + 1, :] + coef * (
            total[5:6, at : at + CH] + total[6:7, at : at + CH]
        )


def call(kernel, shapes, args, scratch=(), flops=0, mib=8):
    return pl.pallas_call(
        kernel,
        out_shape=[jax.ShapeDtypeStruct(s, d) for s, d in shapes],
        in_specs=[VMEM] * len(args),
        out_specs=[VMEM] * len(shapes),
        scratch_shapes=[pltpu.VMEM(s, d) for s, d in scratch],
        cost_estimate=pl.CostEstimate(flops=flops, bytes_accessed=flops // 1000, transcendentals=0),
        compiler_params=pltpu.CompilerParams(vmem_limit_bytes=mib * 2**20),
    )(*args)


def swap(x):
    return lax.ppermute(x, "c", [(0, 1), (1, 0)])


def along(x, d):
    pairs = []
    for chip in range(64):
        pairs.append((2 * chip, 2 * ((chip + d) % 64)))
        pairs.append((2 * chip + 1, 2 * ((chip - d) % 64) + 1))
    return lax.ppermute(x, SPACE, pairs)


def per_device(activations, out_grads, old_input_factor, old_grad_factor):
    images, rows_here, columns_here, _ = activations.shape
    positions = images * lax.axis_size("dp") * rows_here * lax.axis_size(SPACE) * columns_here
    a = activations.reshape(ROW, CH)
    g = out_grads.reshape(ROW, CH)
    a_oth = swap(a)
    g_oth = swap(g)
    own = jnp.concatenate([a, g], axis=0)
    *sent, pair, mine = call(
        prep_kernel,
        [((rows, CH), BF16) for rows in (288, 320, 288, 2 * ROW)] + [((32, CH), F32)],
        (own, a_oth, g_oth),
        scratch=[((CH, CH), F32)],
        flops=1_000_000_000,
    )
    moved = [along(x, d) for d, x in enumerate(sent, 1)]
    moved.append(along(moved[1], 2))
    r1, r2, r3, r4 = moved
    acc, sel = call(
        near_kernel,
        [((2 * M, KK), F32), ((9, 2 * M, CH), BF16)],
        (pair, r1, r2),
        scratch=[((3, 6 * ROW, CH), BF16), ((3, 2 * M, 4 * ROW), BF16)],
        flops=2_000_000_000,
        mib=16,
    )
    (acc,) = call(
        middle_kernel,
        [((2 * M, KK), F32)],
        (r2, r3, sel, acc),
        scratch=[((3, 4 * ROW, CH), BF16), ((3, 2 * M, 2 * ROW), BF16)],
        flops=1_000_000_000,
        mib=16,
    )
    tail = [((3, M, 2 * ROW), BF16), ((16, 8, EXT), F32)]
    give, v, gs = call(
        far_give_kernel,
        [((16, 8, WIDE), BF16), ((3, 4 * ROW, CH), BF16), ((32, CH), F32)],
        (r1, r2, r3, r4, mine, sel, acc),
        scratch=tail,
        flops=1_000_000_000,
        mib=14,
    )
    got = swap(give)
    (keep,) = call(
        far_keep_kernel,
        [((16, 8, WIDE), F32)],
        (sel, acc, v, gs),
        scratch=tail,
        flops=1_000_000_000,
        mib=14,
    )
    (parts,) = call(join_kernel, [((16, 8, WIDE), BF16)], (keep, got))
    arrived = lax.all_to_all(parts, Q, 0, 0, tiled=True)
    return tuple(
        call(
            lambda *refs: end_kernel(0.5 / positions, *refs),
            [((9, KK), F32), ((2, CH), F32)],
            (arrived, old_input_factor, old_grad_factor),
        )
    )


def solution(mesh):
    finer = Mesh(
        mesh.devices.reshape(mesh.shape["dp"], 4, 2, 8, 2),
        ("dp", "y", "xh", "z", "c"),
    )

    return jax.shard_map(
        per_device,
        mesh=finer,
        in_specs=(
            P("dp", SPACE, None, None),
            P("dp", SPACE, None, None),
            P(DP_SPACE, None),
            P(SPACE, None),
        ),
        out_specs=(P(DP_SPACE, None), P(SPACE, None)),
        check_vma=False,
    )
```

```python
import jax
import jax.numpy as jnp
from jax import lax
from jax.experimental import pallas as pl
from jax.experimental.pallas import tpu as pltpu
from jax.sharding import Mesh
from jax.sharding import PartitionSpec as P


SPACE = ("y", "xh", "z", "c")
DP_SPACE = ("dp", "y", "xh", "z", "c")
Q = ("dp", "y", "xh")
ROW = 128
CH = 256
KK = 9 * CH
F32 = jnp.float32
BF16 = jnp.bfloat16
EXT = 512
WIDE = KK + EXT
M = 144

VMEM = pl.BlockSpec(memory_space=pltpu.VMEM)


def here():
    return lax.axis_index("z"), lax.axis_index("c")


def routes(i):
    sends = {}
    for z in range(8):
        side = 1 if z < 4 else -1
        for c in range(2):
            step = side * (i + 4 * c)
            sends.setdefault((z + step) % 8, []).append((z, c, step))
    table = []
    for source in range(8):
        table.append([])
        for z, c, step in sorted(sends[source]):
            table[-1].append((z, c, step))
    return table


def prep_kernel(own, a_oth, g_oth, out1, out2, out3, out4, pair, mine, sums):
    z, c = here()
    a0 = own[:ROW, :]
    a1 = a_oth[...]
    even = jnp.where(c == 0, a0, a1)
    odd = jnp.where(c == 0, a1, a0)
    g = jnp.concatenate([own[ROW:, :], g_oth[...]], axis=0)
    i = lax.broadcasted_iota(jnp.int32, (CH, CH), 0)
    m = lax.broadcasted_iota(jnp.int32, (CH, CH), 1)
    source = 32 * ((m % 32) // 4) + 4 * (m // 32) + m % 4
    by_chip = jnp.where(i == source, 1.0, 0.0).astype(BF16)
    ordered = jnp.dot(g, by_chip, preferred_element_type=F32).astype(BF16)
    sums[...] = lax.dot_general(ordered, g, (((0,), (0,)), ((), ())), preferred_element_type=F32)

    def piece(chip):
        return sums[pl.ds(pl.multiple_of((chip % 8) * 32, 32), 32), :]

    def target(i):
        found = 0
        for source, two in enumerate(routes(i)):
            for core, (to, _, _) in enumerate(two):
                found = jnp.where((z == source) & (c == core), to, found)
        return found

    for i, out in ((1, out1), (2, out2), (3, out3), (4, out4)):
        out[:ROW, :] = even
        out[ROW : 2 * ROW, :] = odd
        out[2 * ROW :, :] = piece(target(i)).astype(BF16)
    pair[:ROW, :] = even
    pair[ROW:, :] = odd
    mine[...] = piece(z)


def shifts(x):
    pos = lax.broadcasted_iota(jnp.int32, (ROW, CH), 0) % 64
    xf = x.astype(F32)
    return (
        jnp.where(pos == 0, 0.0, pltpu.roll(xf, 1, 0)).astype(BF16),
        x,
        jnp.where(pos == 63, 0.0, pltpu.roll(xf, ROW - 1, 0)).astype(BF16),
    )


def selection(t):
    z, c = here()
    m = lax.broadcasted_iota(jnp.int32, (2 * M, CH), 0)
    lane = lax.broadcasted_iota(jnp.int32, (2 * M, CH), 1)
    core = jnp.where(m < M, c, 1 - c)
    m = jnp.where(m < M, m, m - M)
    owner = jnp.where(m < 128, m // 8, m - 128)
    within = jnp.where(m < 128, m % 8, 8)
    channel = owner * M + within + (z * 2 + core) * 9 - lane
    return jnp.where(channel == t * CH, 1.0, 0.0).astype(BF16)


def nt(a, b):
    return lax.dot_general(a, b, (((1,), (1,)), ((), ())), preferred_element_type=F32)


def fill(pairs, v):
    z, _ = here()
    for i, pair in enumerate(pairs):
        at = jnp.where(z < 4, i, len(pairs) - 1 - i)
        for half in range(2):
            where = pl.ds(pl.multiple_of((2 * at + half) * ROW, ROW), ROW)
            for kx, moved in enumerate(shifts(pair[half * ROW : half * ROW + ROW, :])):
                v[kx, where, :] = moved


def left_side(near, pairs, v, sel, lt, first=0, count=2 * M):
    z, c = here()
    chip = (lax.axis_index("y") * 2 + lax.axis_index("xh")) * 8 + z
    patches = 2 * pairs - 2
    step = 4 * c + near
    start = 2 * chip + 1 + 2 * jnp.where(z < 4, step, 1 - step - pairs)
    top = (256 - start) % 128
    bottom = (255 - start) % 128
    lane = lax.broadcasted_iota(jnp.int32, (count, 256), 1)
    for n in range(patches // 2):
        sums = []
        for ky in range(3):
            acc = None
            for kx in range(3):
                part = nt(
                    sel[3 * ky + kx, first : first + count, :],
                    v[kx, ky * ROW + n * 256 : ky * ROW + n * 256 + 256, :],
                )
                acc = part if acc is None else acc + part
            sums.append(acc)
        row = 2 * n + lane // ROW
        at_top = row == top
        at_bottom = row == bottom
        left = jnp.where(at_top, 0.0, sums[0]) + sums[1] + jnp.where(at_bottom, 0.0, sums[2])
        lanes = slice(n * 256, n * 256 + 256)
        lt[0, :, lanes] = jnp.where(at_top, 0.0, left).astype(BF16)
        lt[1, :, lanes] = left.astype(BF16)
        lt[2, :, lanes] = jnp.where(at_bottom, 0.0, left).astype(BF16)


def product(t, patches, v, lt):
    ky, kx = divmod(t, 3)
    return jnp.dot(lt[ky], v[kx, ky * ROW : (ky + patches) * ROW, :], preferred_element_type=F32)


def edges_kernel(pair, mid, r1, r3, r4, acc, sel, v1, v2, lt1, lt2):
    _, c = here()
    first = jnp.where(c == 0, pair[...], mid[: 2 * ROW, :])
    fill((first, r1), v1)
    fill((r3, r4), v2)
    for t in range(9):
        sel[t] = selection(t)
    left_side(0, 2, v1, sel, lt1)
    left_side(3, 2, v2, sel, lt2)
    for t in range(9):
        acc[:, t * CH : t * CH + CH] = product(t, 2, v1, lt1) + product(t, 2, v2, lt2)


def far_give_kernel(r1, r2, r3, r4, mine, sel, old, give, v, gs, lt, ext):
    c = lax.axis_index("c")
    fill((r1, r2, r3), v)
    left_side(1, 3, v, sel, lt, M, M)
    total = jnp.where(c == 0, mine[...], 0.0)
    for ref in (r1, r2, r3):
        total += ref[2 * ROW : 2 * ROW + 32, :].astype(F32)
    gs[...] = total + jnp.where(c == 0, r4[2 * ROW :, :].astype(F32), 0.0)
    finish(1 - c, M, old, v, lt, gs, give, ext)


def far_keep_kernel(sel, old, v, gs, keep, lt, ext):
    left_side(1, 3, v, sel, lt, 0, M)
    finish(lax.axis_index("c"), 0, old, v, lt, gs, keep, ext)


def finish(core, first, old, v, lt, gs, out, ext):
    ext[...] = jnp.zeros_like(ext)
    for t in range(9):
        lanes = slice(t * CH, t * CH + CH)
        res = old[first : first + M, lanes] + product(t, 4, v, lt)
        out[:, :, lanes] = res[:128].reshape(16, 8, CH).astype(out.dtype)
        lanes = slice((t % 2) * CH, (t % 2) * CH + CH)
        for q in range(16):
            ext[q, t // 2 : t // 2 + 1, lanes] = res[128 + q : 129 + q]
    for q in range(8):
        for r in range(2):
            row = gs[pl.ds(q * 4 + r + 2 * core, 1), :]
            high = row.astype(BF16).astype(F32)
            for group in (0, 8):
                ext[group + q, 5:6, r * CH : r * CH + CH] = high
                ext[group + q, 6:7, r * CH : r * CH + CH] = row - high
    out[:, :, KK:] = ext[...].astype(out.dtype)


def join_kernel(keep, got, out):
    for q in range(16):
        total = keep[q] + got[q].astype(F32)
        out[q, :, :] = total.astype(BF16)
        grad = total[5:6, KK:] + total[6:7, KK:]
        high = grad.astype(BF16).astype(F32)
        row = lax.broadcasted_iota(jnp.int32, (8, EXT), 0)
        tail = jnp.where(row == 5, high, jnp.where(row == 6, grad - high, total[:, KK:]))
        out[q, :, KK:] = tail.astype(BF16)


def end_kernel(coef, got, old_in, old_g, out_in, out_g):
    total = got[0].astype(F32)
    for q in range(1, 16):
        total += got[q].astype(F32)
    out_in[0:8, :] = 0.5 * old_in[0:8, :].astype(F32) + coef * total[:, :KK]
    last = 0.5 * old_in[8:9, :].astype(F32)
    for i in range(9):
        at = KK + (i % 2) * CH
        out_in[8:9, i * CH : i * CH + CH] = (
            last[:, i * CH : i * CH + CH] + coef * total[i // 2 : i // 2 + 1, at : at + CH]
        )
    for r in range(2):
        at = KK + r * CH
        out_g[r : r + 1, :] = 0.5 * old_g[r : r + 1, :] + coef * (
            total[5:6, at : at + CH] + total[6:7, at : at + CH]
        )


def call(kernel, shapes, args, scratch=(), flops=0, mib=8):
    return pl.pallas_call(
        kernel,
        out_shape=[jax.ShapeDtypeStruct(s, d) for s, d in shapes],
        in_specs=[VMEM] * len(args),
        out_specs=[VMEM] * len(shapes),
        scratch_shapes=[pltpu.VMEM(s, d) for s, d in scratch],
        cost_estimate=pl.CostEstimate(flops=flops, bytes_accessed=flops // 1000, transcendentals=0),
        compiler_params=pltpu.CompilerParams(vmem_limit_bytes=mib * 2**20),
    )(*args)


def swap(x):
    return lax.ppermute(x, "c", [(0, 1), (1, 0)])


def along(x, i):
    pairs = []
    for two in routes(i):
        for core, (z, c, step) in enumerate(two):
            for q in range(8):
                target = 8 * q + z
                pairs.append((2 * ((target + step) % 64) + core, 2 * target + c))
    return lax.ppermute(x, SPACE, pairs)


def per_device(activations, out_grads, old_input_factor, old_grad_factor):
    images, rows_here, columns_here, _ = activations.shape
    positions = images * lax.axis_size("dp") * rows_here * lax.axis_size(SPACE) * columns_here
    a = activations.reshape(ROW, CH)
    g = out_grads.reshape(ROW, CH)
    a_oth = swap(a)
    g_oth = swap(g)
    own = jnp.concatenate([a, g], axis=0)
    *sent, pair, mine = call(
        prep_kernel,
        [((rows, CH), BF16) for rows in (288, 288, 288, 288, 2 * ROW)] + [((32, CH), F32)],
        (own, a_oth, g_oth),
        scratch=[((CH, CH), F32)],
        flops=1_000_000_000,
    )
    r1, r2, r3, r4 = (along(x, i) for i, x in enumerate(sent, 1))
    mid = swap(r4)
    acc, sel = call(
        edges_kernel,
        [((2 * M, KK), F32), ((9, 2 * M, CH), BF16)],
        (pair, mid, r1, r3, r4),
        scratch=[((3, 4 * ROW, CH), BF16)] * 2 + [((3, 2 * M, 2 * ROW), BF16)] * 2,
        flops=2_000_000_000,
        mib=16,
    )
    tail = [((3, M, 4 * ROW), BF16), ((16, 8, EXT), F32)]
    give, v, gs = call(
        far_give_kernel,
        [((16, 8, WIDE), BF16), ((3, 6 * ROW, CH), BF16), ((32, CH), F32)],
        (r1, r2, r3, r4, mine, sel, acc),
        scratch=tail,
        flops=1_000_000_000,
        mib=14,
    )
    got = swap(give)
    (keep,) = call(
        far_keep_kernel,
        [((16, 8, WIDE), F32)],
        (sel, acc, v, gs),
        scratch=tail,
        flops=1_000_000_000,
        mib=14,
    )
    (parts,) = call(join_kernel, [((16, 8, WIDE), BF16)], (keep, got))
    arrived = lax.all_to_all(parts, Q, 0, 0, tiled=True)
    return tuple(
        call(
            lambda *refs: end_kernel(0.5 / positions, *refs),
            [((9, KK), F32), ((2, CH), F32)],
            (arrived, old_input_factor, old_grad_factor),
        )
    )


def solution(mesh):
    finer = Mesh(
        mesh.devices.reshape(mesh.shape["dp"], 4, 2, 8, 2),
        ("dp", "y", "xh", "z", "c"),
    )

    return jax.shard_map(
        per_device,
        mesh=finer,
        in_specs=(
            P("dp", SPACE, None, None),
            P("dp", SPACE, None, None),
            P(DP_SPACE, None),
            P(SPACE, None),
        ),
        out_specs=(P(DP_SPACE, None), P(SPACE, None)),
        check_vma=False,
    )
```

```python
import jax
import jax.numpy as jnp
from jax import lax
from jax.experimental import pallas as pl
from jax.experimental.pallas import tpu as pltpu
from jax.sharding import Mesh
from jax.sharding import PartitionSpec as P


SPACE = ("y", "xh", "z", "c")
DP_SPACE = ("dp", "y", "xh", "z", "c")
Q = ("dp", "y", "xh")
ROW = 128
CH = 256
KK = 9 * CH
F32 = jnp.float32
BF16 = jnp.bfloat16
EXT = 512
WIDE = KK + EXT
M = 144

VMEM = pl.BlockSpec(memory_space=pltpu.VMEM)


def here():
    return lax.axis_index("z"), lax.axis_index("c")


def routes(i):
    sends = {}
    for z in range(8):
        side = 1 if z < 4 else -1
        for c in range(2):
            step = side * (i + 4 * c)
            sends.setdefault((z + step) % 8, []).append((z, c, step))
    table = []
    for source in range(8):
        table.append([])
        for z, c, step in sorted(sends[source]):
            table[-1].append((z, c, step))
    return table


def prep_kernel(own, a_oth, g_oth, out1, out2, out3, out4, pair, mine, sums):
    z, c = here()
    a0 = own[:ROW, :]
    a1 = a_oth[...]
    even = jnp.where(c == 0, a0, a1)
    odd = jnp.where(c == 0, a1, a0)
    g = jnp.concatenate([own[ROW:, :], g_oth[...]], axis=0)
    i = lax.broadcasted_iota(jnp.int32, (CH, CH), 0)
    m = lax.broadcasted_iota(jnp.int32, (CH, CH), 1)
    source = 32 * ((m % 32) // 4) + 4 * (m // 32) + m % 4
    by_chip = jnp.where(i == source, 1.0, 0.0).astype(BF16)
    ordered = jnp.dot(g, by_chip, preferred_element_type=F32).astype(BF16)
    sums[...] = lax.dot_general(ordered, g, (((0,), (0,)), ((), ())), preferred_element_type=F32)

    def piece(chip):
        return sums[pl.ds(pl.multiple_of((chip % 8) * 32, 32), 32), :]

    def target(i):
        found = 0
        for source, two in enumerate(routes(i)):
            for core, (to, _, _) in enumerate(two):
                found = jnp.where((z == source) & (c == core), to, found)
        return found

    for i, out in ((1, out1), (2, out2), (3, out3), (4, out4)):
        out[:ROW, :] = even
        out[ROW : 2 * ROW, :] = odd
        out[2 * ROW :, :] = piece(target(i)).astype(BF16)
    pair[:ROW, :] = even
    pair[ROW:, :] = odd
    mine[...] = piece(z)


def shifts(x):
    pos = lax.broadcasted_iota(jnp.int32, (ROW, CH), 0) % 64
    xf = x.astype(F32)
    return (
        jnp.where(pos == 0, 0.0, pltpu.roll(xf, 1, 0)).astype(BF16),
        x,
        jnp.where(pos == 63, 0.0, pltpu.roll(xf, ROW - 1, 0)).astype(BF16),
    )


def selection(t):
    z, c = here()
    m = lax.broadcasted_iota(jnp.int32, (2 * M, CH), 0)
    lane = lax.broadcasted_iota(jnp.int32, (2 * M, CH), 1)
    core = jnp.where(m < M, c, 1 - c)
    m = jnp.where(m < M, m, m - M)
    owner = jnp.where(m < 128, m // 8, m - 128)
    within = jnp.where(m < 128, m % 8, 8)
    channel = owner * M + within + (z * 2 + core) * 9 - lane
    return jnp.where(channel == t * CH, 1.0, 0.0).astype(BF16)


def nt(a, b):
    return lax.dot_general(a, b, (((1,), (1,)), ((), ())), preferred_element_type=F32)


def fill(pairs, v):
    z, _ = here()
    for i, pair in enumerate(pairs):
        at = jnp.where(z < 4, i, len(pairs) - 1 - i)
        for half in range(2):
            where = pl.ds(pl.multiple_of((2 * at + half) * ROW, ROW), ROW)
            for kx, moved in enumerate(shifts(pair[half * ROW : half * ROW + ROW, :])):
                v[kx, where, :] = moved


def left_side(near, pairs, v, sel, lt, first=0, count=2 * M):
    z, c = here()
    chip = (lax.axis_index("y") * 2 + lax.axis_index("xh")) * 8 + z
    patches = 2 * pairs - 2
    step = 4 * c + near
    start = 2 * chip + 1 + 2 * jnp.where(z < 4, step, 1 - step - pairs)
    top = (256 - start) % 128
    bottom = (255 - start) % 128
    lane = lax.broadcasted_iota(jnp.int32, (count, 256), 1)
    for n in range(patches // 2):
        sums = []
        for ky in range(3):
            acc = None
            for kx in range(3):
                part = nt(
                    sel[3 * ky + kx, first : first + count, :],
                    v[kx, ky * ROW + n * 256 : ky * ROW + n * 256 + 256, :],
                )
                acc = part if acc is None else acc + part
            sums.append(acc)
        row = 2 * n + lane // ROW
        at_top = row == top
        at_bottom = row == bottom
        left = jnp.where(at_top, 0.0, sums[0]) + sums[1] + jnp.where(at_bottom, 0.0, sums[2])
        lanes = slice(n * 256, n * 256 + 256)
        lt[0, :, lanes] = jnp.where(at_top, 0.0, left).astype(BF16)
        lt[1, :, lanes] = left.astype(BF16)
        lt[2, :, lanes] = jnp.where(at_bottom, 0.0, left).astype(BF16)


def product(t, patches, v, lt):
    ky, kx = divmod(t, 3)
    return jnp.dot(lt[ky], v[kx, ky * ROW : (ky + patches) * ROW, :], preferred_element_type=F32)


def sel_kernel(sel):
    for t in range(9):
        sel[t] = selection(t)


def edges_kernel(pair, mid, r1, r3, r4, sel, acc, v1, v2, lt1, lt2):
    _, c = here()
    first = jnp.where(c == 0, pair[...], mid[: 2 * ROW, :])
    fill((first, r1), v1)
    fill((r3, r4), v2)
    left_side(0, 2, v1, sel, lt1)
    left_side(3, 2, v2, sel, lt2)
    for t in range(9):
        acc[:, t * CH : t * CH + CH] = product(t, 2, v1, lt1) + product(t, 2, v2, lt2)


def far_give_kernel(r1, r2, r3, r4, mine, sel, old, give, v, gs, lt, ext):
    c = lax.axis_index("c")
    fill((r1, r2, r3), v)
    left_side(1, 3, v, sel, lt, M, M)
    total = jnp.where(c == 0, mine[...], 0.0)
    for ref in (r1, r2, r3):
        total += ref[2 * ROW : 2 * ROW + 32, :].astype(F32)
    gs[...] = total + jnp.where(c == 0, r4[2 * ROW :, :].astype(F32), 0.0)
    finish(1 - c, M, old, v, lt, gs, give, ext)


def far_keep_kernel(sel, old, v, gs, keep, lt, ext):
    left_side(1, 3, v, sel, lt, 0, M)
    finish(lax.axis_index("c"), 0, old, v, lt, gs, keep, ext)


def finish(core, first, old, v, lt, gs, out, ext):
    ext[...] = jnp.zeros_like(ext)
    for t in range(9):
        lanes = slice(t * CH, t * CH + CH)
        res = old[first : first + M, lanes] + product(t, 4, v, lt)
        out[:, :, lanes] = res[:128].reshape(16, 8, CH).astype(out.dtype)
        lanes = slice((t % 2) * CH, (t % 2) * CH + CH)
        for q in range(16):
            ext[q, t // 2 : t // 2 + 1, lanes] = res[128 + q : 129 + q]
    for q in range(8):
        for r in range(2):
            row = gs[pl.ds(q * 4 + r + 2 * core, 1), :]
            high = row.astype(BF16).astype(F32)
            for group in (0, 8):
                ext[group + q, 5:6, r * CH : r * CH + CH] = high
                ext[group + q, 6:7, r * CH : r * CH + CH] = row - high
    out[:, :, KK:] = ext[...].astype(out.dtype)


def join_kernel(keep, got, out):
    for q in range(16):
        total = keep[q] + got[q].astype(F32)
        out[q, :, :] = total.astype(BF16)
        grad = total[5:6, KK:] + total[6:7, KK:]
        high = grad.astype(BF16).astype(F32)
        row = lax.broadcasted_iota(jnp.int32, (8, EXT), 0)
        tail = jnp.where(row == 5, high, jnp.where(row == 6, grad - high, total[:, KK:]))
        out[q, :, KK:] = tail.astype(BF16)


def end_kernel(coef, got, old_in, old_g, out_in, out_g):
    total = got[0].astype(F32)
    for q in range(1, 16):
        total += got[q].astype(F32)
    out_in[0:8, :] = 0.5 * old_in[0:8, :].astype(F32) + coef * total[:, :KK]
    last = 0.5 * old_in[8:9, :].astype(F32)
    for i in range(9):
        at = KK + (i % 2) * CH
        out_in[8:9, i * CH : i * CH + CH] = (
            last[:, i * CH : i * CH + CH] + coef * total[i // 2 : i // 2 + 1, at : at + CH]
        )
    for r in range(2):
        at = KK + r * CH
        out_g[r : r + 1, :] = 0.5 * old_g[r : r + 1, :] + coef * (
            total[5:6, at : at + CH] + total[6:7, at : at + CH]
        )


def call(kernel, shapes, args, scratch=(), flops=0, mib=8):
    return pl.pallas_call(
        kernel,
        out_shape=[jax.ShapeDtypeStruct(s, d) for s, d in shapes],
        in_specs=[VMEM] * len(args),
        out_specs=[VMEM] * len(shapes),
        scratch_shapes=[pltpu.VMEM(s, d) for s, d in scratch],
        cost_estimate=pl.CostEstimate(flops=flops, bytes_accessed=flops // 1000, transcendentals=0),
        compiler_params=pltpu.CompilerParams(vmem_limit_bytes=mib * 2**20),
    )(*args)


def swap(x):
    return lax.ppermute(x, "c", [(0, 1), (1, 0)])


def along(x, i):
    pairs = []
    for two in routes(i):
        for core, (z, c, step) in enumerate(two):
            for q in range(8):
                target = 8 * q + z
                pairs.append((2 * ((target + step) % 64) + core, 2 * target + c))
    return lax.ppermute(x, SPACE, pairs)


def per_device(activations, out_grads, old_input_factor, old_grad_factor):
    images, rows_here, columns_here, _ = activations.shape
    positions = images * lax.axis_size("dp") * rows_here * lax.axis_size(SPACE) * columns_here
    a = activations.reshape(ROW, CH)
    g = out_grads.reshape(ROW, CH)
    a_oth = swap(a)
    g_oth = swap(g)
    own = jnp.concatenate([a, g], axis=0)
    *sent, pair, mine = call(
        prep_kernel,
        [((rows, CH), BF16) for rows in (288, 288, 288, 288, 2 * ROW)] + [((32, CH), F32)],
        (own, a_oth, g_oth),
        scratch=[((CH, CH), F32)],
        flops=1_000_000_000,
    )
    r1, r2, r3, r4 = (along(x, i) for i, x in enumerate(sent, 1))
    mid = swap(r4)
    (sel,) = call(sel_kernel, [((9, 2 * M, CH), BF16)], ())
    (acc,) = call(
        edges_kernel,
        [((2 * M, KK), F32)],
        (pair, mid, r1, r3, r4, sel),
        scratch=[((3, 4 * ROW, CH), BF16)] * 2 + [((3, 2 * M, 2 * ROW), BF16)] * 2,
        flops=2_000_000_000,
        mib=16,
    )
    tail = [((3, M, 4 * ROW), BF16), ((16, 8, EXT), F32)]
    give, v, gs = call(
        far_give_kernel,
        [((16, 8, WIDE), BF16), ((3, 6 * ROW, CH), BF16), ((32, CH), F32)],
        (r1, r2, r3, r4, mine, sel, acc),
        scratch=tail,
        flops=1_000_000_000,
        mib=14,
    )
    got = swap(give)
    (keep,) = call(
        far_keep_kernel,
        [((16, 8, WIDE), F32)],
        (sel, acc, v, gs),
        scratch=tail,
        flops=1_000_000_000,
        mib=14,
    )
    (parts,) = call(join_kernel, [((16, 8, WIDE), BF16)], (keep, got))
    arrived = lax.all_to_all(parts, Q, 0, 0, tiled=True)
    return tuple(
        call(
            lambda *refs: end_kernel(0.5 / positions, *refs),
            [((9, KK), F32), ((2, CH), F32)],
            (arrived, old_input_factor, old_grad_factor),
        )
    )


def solution(mesh):
    finer = Mesh(
        mesh.devices.reshape(mesh.shape["dp"], 4, 2, 8, 2),
        ("dp", "y", "xh", "z", "c"),
    )

    return jax.shard_map(
        per_device,
        mesh=finer,
        in_specs=(
            P("dp", SPACE, None, None),
            P("dp", SPACE, None, None),
            P(DP_SPACE, None),
            P(SPACE, None),
        ),
        out_specs=(P(DP_SPACE, None), P(SPACE, None)),
        check_vma=False,
    )
```
